32 devices in a mesh: dp: 2 (over core), expert: 4 (over y, x), mp: 4 (over z).
Axes of the slice: x: 2, y: 2, z: 4, core: 2. Of those that a mesh axis runs over, the one named last changes fastest.
Arguments:
- hidden: bfloat16 [3072, 2, 7168], P(('dp', 'expert'), None, 'mp'), may hold values from -6 to 6
- cotangent: bfloat16 [3072, 2048], P(('dp', 'expert'), 'mp'), may hold values from -6 to 6
- routes: int32 [3072, 2], P(('dp', 'expert')), may hold values from 0 to 3, all different within a row; in each aligned block of 384 rows (0 to 383, 384 to 767, ...) at most 288 rows name the same one
- combine: float32 [3072, 2], P(('dp', 'expert')), may hold values from 0.1 to 0.9
- block_pair: int32 [8, 12], P(('dp', 'expert')), may hold values from 0 to 11, each once within a row
- lengths: int32 [8, 12], P(('dp', 'expert')), may hold values from 4 to 32
- log_ratio: float32 [8, 12], P(('dp', 'expert')), may hold values from -30 to 30
Outputs:
- grad_down: float32 [4, 7168, 2048], P('expert', ('mp', 'dp'))
- expert_load: float32 [4], replicated
The draws below stay inside these ranges and needn't reach their ends.
Inputs may be any that keep to these rules, and one draw needn't show every extreme that they name: `routes`: each row names 2 different experts; in each aligned block of 384 rows (the rows of one device) no expert is named more than 288 times, and in some blocks one expert is named exactly 288 times. `block_pair`: each row holds every number of 0 to 11 once; value v marks the chosen response of the row's pair v // 2 if v is even, its rejected response if v is odd.
All inputs are finite; a program needn't handle non-finite values.
Results may differ from the reference program's by a relative error of at most 0.0029.
Values may be sent and summed in bfloat16 or wider, within the bound.
No kernel may reach another device: no remote copies, remote signals or barrier semaphores. Data moves between devices by JAX's collectives and lax.ppermute only.
A program may use at most 128 MiB of HBM per device.

```python
import math
import jax
import jax.numpy as jnp
import numpy as np
from jax import lax

FFW = 7168
DW = 2048
EXPERTS = 4
TOP = 2
LEN = 32
PAIRS_DEV = 6
TOK_DEV = 384
MOST = 288
GROUPS = 8
TOKENS = 3072
N_DP = 2
N_EXPERT = 4


def draw_lengths(key, part):
    first, second, third = jax.random.split(jax.random.fold_in(key, 17), 3)
    lowest = LEN // 8
    blocks = 2 * PAIRS_DEV
    row_cap = jax.random.randint(first, (GROUPS, 1), lowest, LEN + 1)
    values = jax.random.randint(second, (GROUPS, blocks), lowest, row_cap + 1)
    marked = jax.random.randint(third, (), 0, GROUPS)
    values = values.at[marked, 0].set(LEN)
    values = values.at[(marked + 1) % GROUPS, 1].set(lowest)
    return values.astype(jnp.int32)


def levels(key, dims, cuts, low, high):
    loudness = 1.0
    for axis_at, shards_of in cuts:
        steps = jax.random.uniform(jax.random.fold_in(jax.random.fold_in(key, 6), axis_at), (shards_of,), jnp.float32, low / len(cuts), high / len(cuts))
        loudness = loudness * jnp.repeat(jnp.exp(steps), dims[axis_at] // shards_of).reshape((-1,) + (1,) * (len(dims) - 1 - axis_at))
    return loudness


def deal_out(own_key, own, number, rows, number_of, top, limit, slope):
    sequence = jax.random.permutation(own_key, number_of)
    heavy_load, ordinary = load_shares(number_of, rows * top, limit, slope, True), load_shares(number_of, rows * top, limit, slope, False)
    places = jnp.arange(number_of)

    def named(tallies, rotation):
        used = int((tallies > 0).sum())
        fixed = max(1, used // 4)
        passed = fixed + (places - fixed + rotation * (used - fixed)) % max(1, number_of - fixed)
        return jnp.zeros((number_of,), jnp.int32).at[sequence[jnp.where(places < fixed, places, passed)]].set(jnp.asarray(tallies, jnp.int32))

    tallies = jnp.where(number % 4 == 0, named(heavy_load, number // 4), named(ordinary, number - number // 4 - 1))
    mixed = jax.random.permutation(jax.random.fold_in(own, 3), number_of)
    donor, sink = mixed[0:number_of // 2 * 2:2], mixed[1:number_of // 2 * 2:2]
    slack = jnp.minimum(tallies[donor] - 1, limit - tallies[sink]) // 2
    slack = jnp.where((donor == sequence[0]) | (sink == sequence[0]) | (tallies[sink] == 0), 0, jnp.maximum(slack, 0))
    passed = jax.random.randint(jax.random.fold_in(own, 4), (number_of // 2,), 0, 1 << 20) % (slack + 1)
    tallies = tallies.at[donor].add(-passed).at[sink].add(passed)
    members = jnp.searchsorted(jnp.cumsum(tallies), jnp.arange(rows * top), side="right").astype(jnp.int32)
    listing = members.reshape(top, rows).T
    listing = listing[jax.random.permutation(jax.random.fold_in(own, 1), rows)]
    rotation = jax.random.randint(jax.random.fold_in(own, 2), (rows, 1), 0, top)
    return jnp.take_along_axis(listing, (jnp.arange(top)[None, :] + rotation) % top, axis=1)


def load_shares(number_of, total, limit, slope, full):
    portions = [(1 << 20) // math.isqrt(standing ** slope) + 1 for standing in range(1, number_of + 1)]
    largest = limit if full else min(limit, max(-(-total // number_of), total * portions[0] // sum(portions)))
    least = 1 if total - largest >= number_of - 1 else 0
    counts, surplus = [largest] + [least] * (number_of - 1), total - largest - least * (number_of - 1)
    while surplus > 0:
        movable = [i for i in range(1, number_of) if counts[i] < largest] or [i for i in range(1, number_of) if counts[i] < limit]
        whole, remaining = sum([portions[i] for i in movable]), surplus
        for i in movable:
            addition = min(limit - counts[i], max(1, remaining * portions[i] // whole), surplus)
            counts[i] = counts[i] + addition
            surplus = surplus - addition
    return np.array(counts)


def centred(rng, shape, scale, bound, cuts=(), held_as=jnp.bfloat16):
    level = levels(rng, shape, cuts, -0.22, 0.18) if cuts else 1.0
    values = jax.random.normal(rng, shape, jnp.float32) * scale * level
    return jnp.minimum(jnp.maximum(values, -bound), bound).astype(held_as)


def setup_inputs(seed: int = 0) -> dict:
    splits = jax.random.split(jax.random.key(seed), 8)
    hidden = centred(splits[0], (TOKENS, TOP, FFW), 1.0, 6.0, ((0, 8), (2, 4)))
    cotangent = centred(splits[1], (TOKENS, DW), 1.0, 6.0, ((0, 8), (1, 4)))
    routes_keys = jax.random.split(jax.random.fold_in(splits[2], 1), TOKENS // TOK_DEV)
    routes_turns = jax.random.permutation(jax.random.fold_in(splits[2], 3), TOKENS // TOK_DEV)
    routes = jax.vmap(lambda own, number: deal_out(jax.random.fold_in(splits[2], 2), own, number, TOK_DEV, EXPERTS, TOP, MOST, 2))(routes_keys, routes_turns).reshape((TOKENS, TOP))
    combine = jnp.clip(0.1 + 0.79999997 * jax.random.uniform(splits[3], (TOKENS, TOP), jnp.float32) ** levels(splits[3], (TOKENS, TOP), ((0, 8),), -0.2, 0.2), 0.1, 0.9)
    block_pair = jax.vmap(lambda own: jax.random.permutation(own, 2 * PAIRS_DEV))(jax.random.split(splits[4], GROUPS)).reshape((GROUPS, 2 * PAIRS_DEV)).astype(jnp.int32)
    lengths = draw_lengths(jax.random.fold_in(splits[7], 71), 0)
    log_ratio = jnp.clip(jax.random.uniform(splits[6], (GROUPS, 2 * PAIRS_DEV), jnp.float32, -30.0, 30.0) * levels(splits[6], (GROUPS, 2 * PAIRS_DEV), ((0, 8),), -0.4, 0.0), -30.0, 30.0)
    return dict(hidden=hidden, cotangent=cotangent, routes=routes, combine=combine, block_pair=block_pair, lengths=lengths, log_ratio=log_ratio)


beta_scale = 0.1


def token_weights(combine, block_pair, lengths, log_ratio, block_len):
    blocks = block_pair.shape[1]
    labels = jnp.arange(blocks, dtype=jnp.int32)
    matches = block_pair[:, :, None] == labels[None, None, :]
    by_label = jnp.sum(jnp.where(matches, log_ratio[:, :, None], 0.0), axis=1)
    margin = by_label[:, 0::2] - by_label[:, 1::2]
    pair_coef = beta_scale * jax.nn.sigmoid(-beta_scale * margin)
    owners = block_pair // 2
    pair_ids = jnp.arange(blocks // 2, dtype=jnp.int32)
    picked = owners[:, :, None] == pair_ids[None, None, :]
    block_coef = jnp.sum(jnp.where(picked, pair_coef[:, None, :], 0.0), axis=2)
    block_weight = jnp.where(block_pair % 2 == 0, -block_coef, block_coef)
    position = jnp.arange(block_len, dtype=jnp.int32)
    within = position[None, None, :] < lengths[:, :, None]
    per_token = jnp.where(within, block_weight[:, :, None], 0.0).reshape(-1)
    return combine * per_token[:, None], within.reshape(-1)


def reference(hidden, cotangent, routes, combine, block_pair, lengths, log_ratio):
    weight, within = token_weights(combine, block_pair, lengths, log_ratio, LEN)
    labels = jnp.arange(EXPERTS, dtype=jnp.int32)
    routed = routes[:, :, None] == labels[None, None, :]
    expert_load = jnp.sum(jnp.where(routed & within[:, None, None], 1.0, 0.0), axis=(0, 1)).astype(jnp.float32)
    scaled = (weight[:, :, None] * cotangent[:, None, :].astype(jnp.float32)).astype(jnp.bfloat16)
    slice_rows = TOK_DEV * N_EXPERT * TOP
    room = N_EXPERT * MOST
    hidden_rows = hidden.reshape(N_DP, slice_rows, FFW)
    scaled_rows = scaled.reshape(N_DP, slice_rows, DW)
    route_rows = routes.reshape(N_DP, slice_rows)

    def one_expert(operands, expert_idx):
        slice_hidden, slice_scaled, slice_routes = operands
        chosen = slice_routes == expert_idx
        rank_of = jnp.cumsum(chosen.astype(jnp.int32)) - 1
        target = jnp.where(chosen, rank_of, room)
        source = jnp.zeros((room,), jnp.int32).at[target].set(jnp.arange(slice_rows, dtype=jnp.int32), mode="drop")
        filled = jnp.zeros((room,), jnp.int32).at[target].set(1, mode="drop")
        packed_h = jnp.take(slice_hidden, source, axis=0).astype(jnp.float32)
        packed_s = jnp.where(filled[:, None] > 0, jnp.take(slice_scaled, source, axis=0).astype(jnp.float32), 0.0)
        return jnp.dot(packed_h.T, packed_s, preferred_element_type=jnp.float32)

    def add_slice(running, operands):
        partial_sum = lax.map(lambda expert_idx: one_expert(operands, expert_idx), labels)
        return running + partial_sum, None

    start_total = jnp.zeros((EXPERTS, FFW, DW), jnp.float32)
    grad_down, unused = lax.scan(add_slice, start_total, (hidden_rows, scaled_rows, route_rows))
    return grad_down, expert_load
```

```python
import functools
import jax
import jax.numpy as jnp
from jax import lax
from jax.experimental import pallas as pl
from jax.experimental.pallas import tpu as pltpu
from jax.sharding import PartitionSpec as P

BETA = 0.1
F32 = jnp.float32
BF16 = jnp.bfloat16
VM = pl.BlockSpec(memory_space=pltpu.VMEM)
SM = pl.BlockSpec(memory_space=pltpu.SMEM)
ANY = pl.BlockSpec(memory_space=pl.ANY)


def iota(shape, dim):
    return lax.broadcasted_iota(jnp.int32, shape, dim)


def other(place, hop, size):
    return place ^ hop if size & (size - 1) == 0 else lax.rem(place + hop, size)


def pairs_of(size, hop):
    return [(i, i ^ hop if size & (size - 1) == 0 else (i + hop) % size) for i in range(size)]


def pack_scaled(groups, most, place, routes, combine, pair, lengths, ratio, cot, *outs):
    load, scaled = outs[0], outs[1:]
    blocks = pair.shape[1]
    rows = routes.shape[1]
    length = rows // blocks
    pair_row = jnp.broadcast_to(pair[...], (blocks, blocks))
    ratio_row = jnp.broadcast_to(ratio[...], (blocks, blocks))
    length_row = jnp.broadcast_to(lengths[...], (blocks, blocks))
    eye = iota((blocks, blocks), 0) == iota((blocks, blocks), 1)
    pair_col = jnp.sum(jnp.where(eye, pair_row, 0), axis=1, keepdims=True)
    length_col = jnp.sum(jnp.where(eye, length_row, 0), axis=1, keepdims=True)
    chosen = jnp.sum(jnp.where(pair_row == (pair_col & -2), ratio_row, 0.0), axis=1, keepdims=True)
    refused = jnp.sum(jnp.where(pair_row == (pair_col | 1), ratio_row, 0.0), axis=1, keepdims=True)
    coef = BETA * jax.nn.sigmoid(-BETA * (chosen - refused))
    block_weight = jnp.where((pair_col & 1) == 0, -coef, coef)
    owner = iota((blocks, rows), 1) // length == iota((blocks, rows), 0)
    weight = jnp.sum(jnp.where(owner, block_weight, 0.0), axis=0, keepdims=True)
    valid = jnp.sum(jnp.where(owner, length_col, 0), axis=0, keepdims=True)
    live = iota((1, rows), 1) % length < valid
    weight = jnp.where(live, weight, 0.0)
    first, second = routes[0:1, :], routes[1:2, :]
    weight0, weight1 = combine[0:1, :] * weight, combine[1:2, :] * weight
    pad = -(-groups // 8) * 8
    label = iota((pad, rows), 0)
    counted = ((first == label) | (second == label)) & live
    counts = jnp.sum(jnp.where(counted, 1.0, 0.0), axis=1, keepdims=True)
    load[...] = jnp.broadcast_to(counts, load.shape)
    named = other(jnp.broadcast_to(place[0], (pad, rows)), label, groups)
    hit0, hit1 = first == named, second == named
    hit = hit0 | hit1
    before = jnp.where(iota((rows, rows), 0) < iota((rows, rows), 1), 1.0, 0.0).astype(BF16)
    rank = jnp.dot(jnp.where(hit, 1.0, 0.0).astype(BF16), before, preferred_element_type=F32)
    key = jnp.where(hit, rank, -1.0)
    by_group = jnp.where(hit0, weight0, jnp.where(hit1, weight1, 0.0))
    slot = iota((most, rows), 0).astype(F32)
    for j in range(groups):
        at = slot == key[j : j + 1, :]
        row_weight = jnp.sum(jnp.where(at, by_group[j : j + 1, :], 0.0), axis=1, keepdims=True)
        taken = jnp.dot(jnp.where(at, 1.0, 0.0).astype(BF16), cot[...], preferred_element_type=F32)
        scaled[j][...] = (row_weight * taken).astype(BF16)


def pack_hidden(groups, most, halves, place, routes, hidden, *outs):
    flat = routes.shape[1]
    width = hidden.shape[1] // halves
    pad = -(-groups // 8) * 8
    named = other(jnp.broadcast_to(place[0], (pad, flat)), iota((pad, flat), 0), groups)
    hit = routes[...] == named
    before = jnp.where(iota((flat, flat), 0) < iota((flat, flat), 1), 1.0, 0.0).astype(BF16)
    rank = jnp.dot(jnp.where(hit, 1.0, 0.0).astype(BF16), before, preferred_element_type=F32)
    key = jnp.where(hit, rank, -1.0)
    slot = iota((most, flat), 0).astype(F32)
    for j in range(groups):
        at = jnp.where(slot == key[j : j + 1, :], 1.0, 0.0).astype(BF16)
        for h in range(halves):
            part = other(place[1], h, halves)
            columns = pl.ds(pl.multiple_of(part * width, 128), width)
            taken = jnp.dot(at, hidden[:, columns], preferred_element_type=F32)
            outs[h * groups + j][...] = taken.astype(BF16)


def turn(step, *refs):
    blocks, out, joined = refs[:-2], refs[-2], refs[-1]
    most = blocks[0].shape[0]
    for i, block in enumerate(blocks):
        joined[i * most : (i + 1) * most, :] = block[...]
    for i in range(0, joined.shape[0], step):
        out[:, i : i + step] = joined[i : i + step, :].T


def product(tile, fresh, where_to, ht, mine, theirs, *rest):
    out, total, sem = rest[-3:]
    rows = mine.shape[0]
    width = mine.shape[1]

    @pl.when(where_to[0] > 0)
    def _():
        column = pl.multiple_of(where_to[1] * width, 128)
        copies = []
        for i in range(0, ht.shape[0], tile):
            total[i : i + tile, :] = jnp.dot(
                ht[i : i + tile, :rows], mine[...], preferred_element_type=F32
            ) + jnp.dot(ht[i : i + tile, rows:], theirs[...], preferred_element_type=F32)
            copy = pltpu.make_async_copy(
                total.at[pl.ds(i, tile)],
                out.at[pl.ds(i, tile), pl.ds(column, width)],
                sem.at[i // tile],
            )
            copy.start()
            copies.append(copy)
        for copy in copies:
            copy.wait()


def cost(flops, moved):
    return pl.CostEstimate(flops=flops, bytes_accessed=moved, transcendentals=0)


def body(hidden, cotangent, routes, combine, block_pair, lengths, log_ratio):
    dp, groups, line = (lax.axis_size(name) for name in ("dp", "expert", "mp"))
    d, e, m = (lax.axis_index(name).astype(jnp.int32) for name in ("dp", "expert", "mp"))
    tokens, top = routes.shape
    most = 3 * tokens // 4
    width = cotangent.shape[1]
    inner = hidden.shape[2]
    pair_of_cores = dp == 2
    halves = 2 if pair_of_cores else 1
    part = inner // halves
    place = jnp.stack([e, d])
    routes_t, combine_t = routes.T, combine.T

    packed = pl.pallas_call(
        functools.partial(pack_scaled, groups, most),
        out_shape=[jax.ShapeDtypeStruct((8 * (-(-groups // 8)), 128), F32)]
        + [jax.ShapeDtypeStruct((most, width), BF16)] * groups,
        in_specs=[SM] + [VM] * 6,
        out_specs=[VM] * (groups + 1),
        cost_estimate=cost(2 * groups * most * tokens * width, 4 * most * width * 4),
        name="pack_scaled",
    )(place, routes_t, combine_t, block_pair, lengths, log_ratio, cotangent)
    load, scaled = packed[0], packed[1:]

    packed_h = pl.pallas_call(
        functools.partial(pack_hidden, groups, most, halves),
        out_shape=[jax.ShapeDtypeStruct((most, part), BF16)] * (groups * halves),
        in_specs=[SM, VM, VM],
        out_specs=[VM] * (groups * halves),
        cost_estimate=cost(2 * groups * most * tokens * top * inner, 8 * most * inner * 4),
        name="pack_hidden",
    )(place, routes.reshape(1, tokens * top), hidden.reshape(tokens * top, inner))

    arrived = [scaled[0]] + [
        lax.ppermute(scaled[j], "expert", pairs_of(groups, j)) for j in range(1, groups)
    ]
    blocks = []
    for h in range(halves):
        for j in range(groups):
            block = packed_h[h * groups + j]
            if h:
                block = lax.ppermute(
                    block,
                    ("dp", "expert"),
                    [(a * groups + b, (a ^ h) * groups + c) for a in range(dp) for b, c in pairs_of(groups, j)],
                )
            elif j:
                block = lax.ppermute(block, "expert", pairs_of(groups, j))
            blocks.append(block)

    size = dp * groups
    if size & (size - 1) == 0:
        hop = 1
        while hop < size:
            load = load + lax.ppermute(load, ("dp", "expert"), pairs_of(size, hop))
            hop *= 2
    else:
        load = lax.psum(load, ("dp", "expert"))
    expert_load = load[:groups, 0]

    up = [(i, i + 1) for i in range(line - 1)]
    down = [(i + 1, i) for i in range(line - 1)]
    lead, rest = arrived[0], jnp.concatenate(arrived[1:], axis=0)
    below, above = [(lead, rest)], [(lead, rest)]
    for hop in range(1, line):
        below.append(tuple(lax.ppermute(x, "mp", up[hop - 1 :]) for x in below[-1]))
        above.append(tuple(lax.ppermute(x, "mp", down[: line - hop]) for x in above[-1]))

    shards = [(jnp.concatenate(below[0], axis=0), m * 0 + 1, m)]
    for hop in range(1, line):
        low, high = below[hop], above[hop]
        if 2 * hop < line:
            shards.append((jnp.concatenate(low, axis=0), m >= hop, m - hop))
            shards.append((jnp.concatenate(high, axis=0), m + hop < line, m + hop))
        else:
            both = [jnp.where(m >= hop, a, b) for a, b in zip(low, high)]
            shards.append(
                (
                    jnp.concatenate(both, axis=0),
                    (m >= hop) | (m + hop < line),
                    jnp.where(m >= hop, m - hop, m + hop),
                )
            )

    rows = groups * most
    if not pair_of_cores:
        joined = jnp.concatenate(blocks, axis=0)
        partial = jnp.zeros((inner, width * line), F32)
        for shard, valid, at in shards:
            piece = lax.dot_general(joined, shard, (((0,), (0,)), ((), ())), preferred_element_type=F32)
            at = jnp.clip(at, 0, line - 1) * width
            old = lax.dynamic_slice(partial, (0, at), piece.shape)
            partial = lax.dynamic_update_slice(partial, jnp.where(valid, piece, old), (0, at))
        owned = lax.psum_scatter(partial, "dp", scatter_dimension=0, tiled=True)
        return owned[None], expert_load

    swap = [(0, 1), (1, 0)]
    step = 256 if (2 * rows) % 256 == 0 else most
    ht = pl.pallas_call(
        functools.partial(turn, step),
        out_shape=jax.ShapeDtypeStruct((part, 2 * rows), BF16),
        in_specs=[VM] * len(blocks),
        out_specs=VM,
        scratch_shapes=[pltpu.VMEM((2 * rows, part), BF16)],
        cost_estimate=cost(2 * rows * part * 512, 4 * rows * part * 2),
        name="turn",
    )(*blocks)
    tile = part // 7 if part % (7 * 128) == 0 else part
    out = None
    for shard, valid, at in shards:
        theirs = lax.ppermute(shard, "dp", swap)
        where_to = jnp.stack([jnp.asarray(valid, jnp.int32), at])
        extra = [] if out is None else [out]
        out = pl.pallas_call(
            functools.partial(product, tile, out is None),
            out_shape=jax.ShapeDtypeStruct((part, width * line), F32),
            in_specs=[SM, VM, VM, VM] + [ANY] * len(extra),
            out_specs=ANY,
            input_output_aliases={} if out is None else {4: 0},
            scratch_shapes=[
                pltpu.VMEM((part, width), F32),
                pltpu.SemaphoreType.DMA((part // tile,)),
            ],
            cost_estimate=cost(4 * part * rows * width, part * rows * 4 + part * width * 4),
            name="product",
        )(where_to, ht, shard, theirs, *extra)
    return out[None], expert_load


def solution(mesh):
    in_specs = (
        P(("dp", "expert"), None, "mp"),
        P(("dp", "expert"), "mp"),
        P(("dp", "expert"), None),
        P(("dp", "expert"), None),
        P(("dp", "expert"), None),
        P(("dp", "expert"), None),
        P(("dp", "expert"), None),
    )
    out_specs = (P("expert", ("mp", "dp"), None), P())
    return jax.shard_map(body, mesh=mesh, in_specs=in_specs, out_specs=out_specs, check_vma=False)
```

```python
import functools
import math
import jax
import jax.numpy as jnp
from jax import lax
from jax.experimental import pallas as pl
from jax.experimental.pallas import tpu as pltpu
from jax.sharding import PartitionSpec as P


BETA = 0.1
F32 = jnp.float32
BF16 = jnp.bfloat16
VM = pl.BlockSpec(memory_space=pltpu.VMEM)
ANY = pl.BlockSpec(memory_space=pl.ANY)
HBM = pl.BlockSpec(memory_space=pltpu.HBM)


def iota(shape, dim):
    return lax.broadcasted_iota(jnp.int32, shape, dim)


def other(place, hop, size):
    return place ^ hop if size & (size - 1) == 0 else lax.rem(place + hop, size)


def pairs_of(size, hop):
    return [(i, i ^ hop if size & (size - 1) == 0 else (i + hop) % size) for i in range(size)]


def pack_scaled(groups, most, early, *refs):
    load, ranks, shares, routes, raw = refs[6:11]
    scaled = refs[11 : 11 + groups]
    combine, pair, lengths, ratio, cot, sem = refs[11 + groups :]
    copies = [
        pltpu.make_async_copy(source, held, sem.at[i])
        for i, (source, held) in enumerate(zip(refs[:6], (routes, combine, pair, lengths, ratio, cot)))
    ]
    for copy in copies:
        copy.start()
    for copy in copies:
        copy.wait()
    blocks = pair.shape[1]
    rows = routes.shape[1]
    length = rows // blocks
    pair_row = jnp.broadcast_to(pair[...], (blocks, blocks))
    ratio_row = jnp.broadcast_to(ratio[...], (blocks, blocks))
    length_row = jnp.broadcast_to(lengths[...], (blocks, blocks))
    eye = iota((blocks, blocks), 0) == iota((blocks, blocks), 1)
    pair_col = jnp.sum(jnp.where(eye, pair_row, 0), axis=1, keepdims=True)
    length_col = jnp.sum(jnp.where(eye, length_row, 0), axis=1, keepdims=True)
    chosen = jnp.sum(jnp.where(pair_row == (pair_col & -2), ratio_row, 0.0), axis=1, keepdims=True)
    refused = jnp.sum(jnp.where(pair_row == (pair_col | 1), ratio_row, 0.0), axis=1, keepdims=True)
    coef = BETA * jax.nn.sigmoid(-BETA * (chosen - refused))
    block_weight = jnp.where((pair_col & 1) == 0, -coef, coef)
    owner = iota((blocks, rows), 1) // length == iota((blocks, rows), 0)
    weight = jnp.sum(jnp.where(owner, block_weight, 0.0), axis=0, keepdims=True)
    valid = jnp.sum(jnp.where(owner, length_col, 0), axis=0, keepdims=True)
    live = iota((1, rows), 1) % length < valid
    weight = jnp.where(live, weight, 0.0)
    first, second = routes[0:1, :], routes[1:2, :]
    weight0, weight1 = combine[0:1, :] * weight, combine[1:2, :] * weight
    pad = -(-groups // 8) * 8
    label = iota((pad, rows), 0)
    counted = ((first == label) | (second == label)) & live
    counts = jnp.sum(jnp.where(counted, 1.0, 0.0), axis=1, keepdims=True)
    load[...] = jnp.broadcast_to(counts, load.shape)
    named = other(jnp.full((pad, rows), lax.axis_index("expert"), jnp.int32), label, groups)
    hit0, hit1 = first == named, second == named
    hit = hit0 | hit1
    before = jnp.where(iota((rows, rows), 0) < iota((rows, rows), 1), 1.0, 0.0).astype(BF16)
    rank = jnp.dot(jnp.where(hit, 1.0, 0.0).astype(BF16), before, preferred_element_type=F32)
    key = jnp.where(hit, rank, -1.0)
    by_group = jnp.where(hit0, weight0, jnp.where(hit1, weight1, 0.0))
    ranks[...] = key
    shares[...] = by_group
    raw[...] = cot[:, : raw.shape[1]]
    place_scaled(most, key, by_group, cot[:, early:], scaled)


def place_scaled(most, key, by_group, source, outs):
    slot = iota((most, key.shape[1]), 0).astype(F32)
    for j, out in enumerate(outs):
        at = slot == key[j : j + 1, :]
        row_weight = jnp.sum(jnp.where(at, by_group[j : j + 1, :], 0.0), axis=1, keepdims=True)
        taken = jnp.dot(jnp.where(at, 1.0, 0.0).astype(BF16), source, preferred_element_type=F32)
        out[:most, :] = (row_weight * taken).astype(BF16)


def pack_early(most, line, key, by_group, load, *refs):
    source, outs = jnp.concatenate([x[...] for x in refs[:line]], axis=1), refs[line:]
    place_scaled(most, key[...], by_group[...], source, outs)
    counts = split_counts(load[:, :1], source.shape[1])
    for out in outs:
        out[most:, :] = counts


def split_counts(counts, columns):
    high = jnp.floor(counts * (1.0 / 128.0))
    both = jnp.concatenate([high, counts - 128.0 * high], axis=0)
    return jnp.broadcast_to(both, (both.shape[0], columns)).astype(BF16)


def read_counts(rows):
    rows = rows.astype(F32)
    half = rows.shape[0] // 2
    return 128.0 * rows[:half] + rows[half:]


def join_early(most, *refs):
    blocks, out = refs[:-1], refs[-1]
    counts = sum(read_counts(block[most:, :128]) for block in blocks)
    for i, block in enumerate(blocks):
        out[i * most : (i + 1) * most, :] = block[:most, :]
    out[len(blocks) * most :, :] = split_counts(counts[:, :1], out.shape[1])


def tally(rows, mine, theirs, out):
    out[...] = read_counts(mine[rows:, :128]) + read_counts(theirs[rows:, :128])


def pack_hidden(groups, most, hop, halves, routes, key, hidden, *outs):
    rows, top, inner = hidden.shape
    width = inner // halves
    flat = rows * top
    part = other(lax.axis_index("dp"), hop, halves) if halves > 1 else 0
    columns = pl.ds(pl.multiple_of(part * width, 128), width)
    pad = key.shape[0]
    spread = jnp.where(iota((rows, flat), 0) == iota((rows, flat), 1) // top, 1.0, 0.0).astype(BF16)
    high = jnp.floor(key[...] * (1.0 / 16.0))
    low = key[...] - 16.0 * high
    named = [jnp.broadcast_to(routes[k : k + 1, :].astype(F32), (pad, rows)) for k in range(top)]
    stacked = jnp.concatenate([high, low] + named, axis=0).astype(BF16)
    wide = jnp.dot(stacked, spread, preferred_element_type=F32)
    key = 16.0 * wide[:pad] + wide[pad : 2 * pad]
    choice = iota((pad, flat), 1) % top
    route = wide[2 * pad : 3 * pad]
    for k in range(1, top):
        route = jnp.where(choice == k, wide[(2 + k) * pad : (3 + k) * pad], route)
    me = jnp.full((pad, flat), lax.axis_index("expert"), jnp.int32)
    label = other(me, iota((pad, flat), 0), groups).astype(F32)
    key = jnp.where(route == label, key, -1.0)
    slot = iota((most, flat), 0).astype(F32)
    source = hidden[:, :, columns].reshape(flat, width)
    for j in range(groups):
        at = jnp.where(slot == key[j : j + 1, :], 1.0, 0.0).astype(BF16)
        outs[j][...] = jnp.dot(at, source, preferred_element_type=F32).astype(BF16)


def turn(step, *refs):
    blocks, out, joined = refs[:-2], refs[-2], refs[-1]
    most = blocks[0].shape[0]
    for i, block in enumerate(blocks):
        joined[i * most : (i + 1) * most, :] = block[...]
    for i in range(0, joined.shape[0], step):
        out[:, i : i + step] = joined[i : i + step, :].T


def stack_into(out, parts):
    at = 0
    for part in parts:
        out[at : at + part.shape[0], :] = part[...]
        at += part.shape[0]


def join(*refs):
    stack_into(refs[-1], refs[:-1])


def join_either(hop, *refs):
    half = (len(refs) - 1) // 2
    from_below = lax.axis_index("mp") >= hop

    @pl.when(from_below)
    def _():
        stack_into(refs[-1], refs[:half])

    @pl.when(jnp.logical_not(from_below))
    def _():
        stack_into(refs[-1], refs[half:-1])


def arrival(which, hop, line):
    m = lax.axis_index("mp")
    low, high = m >= hop, m + hop < line
    if which == "below":
        return low, m - hop
    if which == "above":
        return high, m + hop
    return low | high, jnp.where(low, m - hop, m + hop)


def half_product(tile, ht, mine, out):
    for i in range(0, ht.shape[0], tile):
        out[i : i + tile, :] = jnp.dot(
            ht[i : i + tile, : mine.shape[0]], mine[...], preferred_element_type=F32
        )


def last_product(tile, line, which, hop, ht, first, theirs, _, out, total, sem):
    rows, width = theirs.shape
    shard = out.shape[1] // line
    valid, at = arrival(which, hop, line)

    @pl.when(valid)
    def _():
        column = pl.multiple_of(at * shard + shard - width, 128)
        copies = []
        for i in range(0, ht.shape[0], tile):
            total[i : i + tile, :] = first[i : i + tile, :] + jnp.dot(
                ht[i : i + tile, rows:], theirs[...], preferred_element_type=F32
            )
            copy = pltpu.make_async_copy(
                total.at[pl.ds(i, tile)],
                out.at[pl.ds(i, tile), pl.ds(column, width)],
                sem.at[i // tile],
            )
            copy.start()
            copies.append(copy)
        for copy in copies:
            copy.wait()


def product(tile, line, steps, ht, *refs):
    sources, (out, joined, total, sem) = refs[: 2 * max(len(steps), 1)], refs[-4:]
    rows, width = ht.shape[1] // 2, sources[0].shape[1]
    shard = out.shape[1] // line
    for k in range(len(sources)):
        at = (k % 2) * rows, (k // 2) * width
        joined[at[0] : at[0] + rows, at[1] : at[1] + width] = sources[k][:rows, :]
    if steps:
        marks = [arrival(which, hop, line) for which, hop in steps]
        marks = [(valid, at * shard + shard - width, width) for valid, at in marks]
    else:
        m = lax.axis_index("mp")
        marks = [(m >= 0, lax.rem(m + line - k, line) * shard, width // line) for k in range(line)]
    tiles = ht.shape[0] // tile

    def write(i, k, act):
        valid, column, size = marks[k]

        @pl.when(valid)
        def _():
            act(
                pltpu.make_async_copy(
                    total.at[pl.ds(i * tile, tile), pl.ds(k * size, size)],
                    out.at[pl.ds(i * tile, tile), pl.ds(pl.multiple_of(column, 128), size)],
                    sem.at[i * len(marks) + k],
                )
            )

    for i in range(tiles):
        total[i * tile : (i + 1) * tile, :] = jnp.dot(
            ht[i * tile : (i + 1) * tile, :], joined[...], preferred_element_type=F32
        )
        for k in range(len(marks)):
            write(i, k, lambda copy: copy.start())
    for i in range(tiles):
        for k in range(len(marks)):
            write(i, k, lambda copy: copy.wait())


def call(kernel, name, outs, specs, mib, flops, scratch=(), alias=None):
    many = isinstance(outs, list)
    moved = sum(math.prod(x.shape) * 4 for x in (outs if many else [outs]))
    return pl.pallas_call(
        kernel,
        out_shape=outs,
        in_specs=specs,
        out_specs=[VM] * len(outs) if many else (ANY if "_product" in name else VM),
        scratch_shapes=list(scratch),
        input_output_aliases=alias or {},
        compiler_params=pltpu.CompilerParams(vmem_limit_bytes=mib << 20),
        cost_estimate=pl.CostEstimate(flops=flops, bytes_accessed=moved, transcendentals=0),
    )


def work(hidden, cotangent, routes, combine, block_pair, lengths, log_ratio):
    dp, groups, line = (lax.axis_size(name) for name in ("dp", "expert", "mp"))
    m = lax.axis_index("mp").astype(jnp.int32)
    tokens, top = routes.shape
    most = 3 * tokens // 4
    full = cotangent.shape[1]
    inner = hidden.shape[2]
    pair_of_cores = dp == 2
    halves = 2 if pair_of_cores else 1
    part = inner // halves
    early = full // 4 if pair_of_cores and full % 512 == 0 else 0
    width = full - early
    rows = groups * most
    pad = 8 * (-(-groups // 8))
    operands = (routes.T, combine.T, block_pair, lengths, log_ratio, cotangent)

    packed = call(
        functools.partial(pack_scaled, groups, most, early),
        "pack_scaled",
        [
            jax.ShapeDtypeStruct((pad, 128), F32),
            jax.ShapeDtypeStruct((pad, tokens), F32),
            jax.ShapeDtypeStruct((pad, tokens), F32),
            jax.ShapeDtypeStruct((top, tokens), jnp.int32),
            jax.ShapeDtypeStruct((tokens, max(early, 128)), BF16),
        ]
        + [jax.ShapeDtypeStruct((most, width), BF16)] * groups,
        [HBM] * 6,
        60,
        2 * groups * most * tokens * width,
        [pltpu.VMEM(x.shape, x.dtype) for x in operands[1:]] + [pltpu.SemaphoreType.DMA((6,))],
    )(*operands)
    load, key, shares, routes_held, raw = packed[:5]
    scaled = packed[5:]

    packed_h = [
        call(
            functools.partial(pack_hidden, groups, most, h, halves),
            f"pack_hidden{h}",
            [jax.ShapeDtypeStruct((most, part), BF16)] * groups,
            [VM, VM, VM],
            24,
            2 * rows * tokens * top * part,
        )(routes_held, key, hidden)
        for h in range(halves)
    ]

    arrived = [scaled[0]] + [
        lax.ppermute(scaled[j], "expert", pairs_of(groups, j)) for j in range(1, groups)
    ]
    blocks = []
    for h in range(halves):
        for j in range(groups):
            block = packed_h[h][j]
            if h:
                block = lax.ppermute(
                    block,
                    ("dp", "expert"),
                    [(a * groups + b, (a ^ h) * groups + c) for a in range(dp) for b, c in pairs_of(groups, j)],
                )
            elif j:
                block = lax.ppermute(block, "expert", pairs_of(groups, j))
            blocks.append(block)

    if not early:
        expert_load = lax.psum(load, ("dp", "expert"))[:groups, 0]

    def joined(name, kernel, *parts):
        count = rows if kernel is not join else sum(x.shape[0] for x in parts)
        return call(
            kernel, name, jax.ShapeDtypeStruct((count, parts[0].shape[1]), BF16), [VM] * len(parts), 8, 0
        )(*parts)

    up = [(i, i + 1) for i in range(line - 1)]
    down = [(i + 1, i) for i in range(line - 1)]
    start = joined("join", join, *arrived)
    below, above = [start], [start]
    for hop in range(1, line):
        below.append(lax.ppermute(below[-1], "mp", up[hop - 1 :]))
        above.append(lax.ppermute(above[-1], "mp", down[: line - hop]))

    shards = [(start, "below", 0)]
    for hop in range(1, line):
        if 2 * hop < line:
            shards.append((below[hop], "below", hop))
            shards.append((above[hop], "above", hop))
        else:
            either = functools.partial(join_either, hop)
            shards.append((joined(f"join{hop}", either, below[hop], above[hop]), "either", hop))

    if not pair_of_cores:
        hidden_rows = jnp.concatenate(blocks, axis=0)
        partial = jnp.zeros((inner, full * line), F32)
        for shard, which, hop in shards:
            piece = lax.dot_general(
                hidden_rows, shard, (((0,), (0,)), ((), ())), preferred_element_type=F32
            )
            low, high = m >= hop, m + hop < line
            valid = {"below": low, "above": high, "either": low | high}[which]
            at = jnp.where(low if which != "above" else False, m - hop, m + hop)
            at = jnp.clip(at, 0, line - 1) * full
            old = lax.dynamic_slice(partial, (0, at), piece.shape)
            partial = lax.dynamic_update_slice(partial, jnp.where(valid, piece, old), (0, at))
        owned = lax.psum_scatter(partial, "dp", scatter_dimension=0, tiled=True)
        return owned[None], expert_load

    step = 256 if (2 * rows) % 256 == 0 else most
    ht = call(
        functools.partial(turn, step),
        "turn",
        jax.ShapeDtypeStruct((part, 2 * rows), BF16),
        [VM] * len(blocks),
        20,
        2 * rows * part * 512,
        [pltpu.VMEM((2 * rows, part), BF16)],
    )(*blocks)
    tile = part // 2 if part % 16 == 0 else part
    out_shape = jax.ShapeDtypeStruct((part, full * line), F32)

    def swap(mine):
        return lax.ppermute(mine, "dp", [(0, 1), (1, 0)])

    def multiply(name, sources, steps, out):
        columns = sources[0].shape[1] * max(len(steps), 1)
        writes = len(steps) or line
        extra = [] if out is None else [out]
        return call(
            functools.partial(product, tile, line, steps),
            name,
            out_shape,
            [VM] * (1 + len(sources)) + [ANY] * len(extra),
            24,
            4 * part * rows * columns,
            [
                pltpu.VMEM((2 * rows, columns), BF16),
                pltpu.VMEM((part, columns), F32),
                pltpu.SemaphoreType.DMA((part // tile * writes,)),
            ],
            {} if out is None else {1 + len(sources): 0},
        )(ht, *sources, *extra)

    have = []
    for mine, which, hop in shards:
        have.append((mine, swap(mine), which, hop))
    out = None
    early_shards = have[:-1]
    first = early_shards[:1] + early_shards[-1:] if len(early_shards) > 1 else early_shards
    for i, group in enumerate((first, early_shards[1:-1])):
        for k in range(0, len(group), 2):
            some = group[k : k + 2]
            sources = [x for mine, theirs, _, _ in some for x in (mine, theirs)]
            steps = tuple((which, hop) for _, _, which, hop in some)
            out = multiply(f"pair_product{i}", sources, steps, out)
    if early:
        spread = [raw] + [
            lax.ppermute(raw, "mp", [(a, (a + k) % line) for a in range(line)])
            for k in range(1, line)
        ]
        sent = call(
            functools.partial(pack_early, most, line),
            "pack_early",
            [jax.ShapeDtypeStruct((most + 2 * pad, early * line), BF16)] * groups,
            [VM] * (3 + line),
            12,
            2 * rows * tokens * early * line,
        )(key, shares, load, *spread)
        kept = [sent[0]] + [
            lax.ppermute(sent[j], "expert", pairs_of(groups, j)) for j in range(1, groups)
        ]
        own = call(
            functools.partial(join_early, most),
            "join_early",
            jax.ShapeDtypeStruct((rows + 2 * pad, early * line), BF16),
            [VM] * groups,
            8,
            0,
        )(*kept)
        theirs = swap(own)
        out = multiply("early_product", [own, theirs], (), out)
        expert_load = call(
            functools.partial(tally, rows),
            "tally",
            jax.ShapeDtypeStruct((pad, 128), F32),
            [VM] * 2,
            8,
            0,
        )(own, theirs)[:groups, 0]
    mine, theirs, which, hop = have[-1]
    half = call(
        functools.partial(half_product, tile),
        "half",
        jax.ShapeDtypeStruct((part, width), F32),
        [VM, VM],
        16,
        2 * part * rows * width,
    )(ht, mine)
    out = call(
        functools.partial(last_product, tile, line, which, hop),
        "last_product",
        out_shape,
        [VM, VM, VM, ANY],
        20,
        2 * part * rows * width,
        [pltpu.VMEM((part, width), F32), pltpu.SemaphoreType.DMA((part // tile,))],
        {3: 0},
    )(ht, half, theirs, out)
    return out[None], expert_load


def solution(mesh):
    in_specs = (
        P(("dp", "expert"), None, "mp"),
        P(("dp", "expert"), "mp"),
        P(("dp", "expert"), None),
        P(("dp", "expert"), None),
        P(("dp", "expert"), None),
        P(("dp", "expert"), None),
        P(("dp", "expert"), None),
    )
    out_specs = (P("expert", ("mp", "dp"), None), P())
    step = jax.shard_map(work, mesh=mesh, in_specs=in_specs, out_specs=out_specs, check_vma=False)
    if tuple(mesh.shape[name] for name in ("dp", "expert", "mp")) != (2, 4, 4):
        return step
    return step
```

```python
import functools
import math
import jax
import jax.numpy as jnp
from jax import lax
from jax.experimental import pallas as pl
from jax.experimental.pallas import tpu as pltpu
from jax.sharding import PartitionSpec as P


BETA = 0.1
F32 = jnp.float32
BF16 = jnp.bfloat16
VM = pl.BlockSpec(memory_space=pltpu.VMEM)
ANY = pl.BlockSpec(memory_space=pl.ANY)
HBM = pl.BlockSpec(memory_space=pltpu.HBM)


def iota(shape, dim):
    return lax.broadcasted_iota(jnp.int32, shape, dim)


def other(place, hop, size):
    return place ^ hop if size & (size - 1) == 0 else lax.rem(place + hop, size)


def pairs_of(size, hop):
    return [(i, i ^ hop if size & (size - 1) == 0 else (i + hop) % size) for i in range(size)]


def pack_scaled(groups, most, early, *refs):
    table, raw = refs[6:8]
    scaled = refs[8 : 8 + groups]
    routes, combine, pair, lengths, ratio, cot, sem = refs[8 + groups :]
    copies = [
        pltpu.make_async_copy(source, held, sem.at[i])
        for i, (source, held) in enumerate(zip(refs[:6], (routes, combine, pair, lengths, ratio, cot)))
    ]
    for copy in copies:
        copy.start()
    for copy in copies[:-1]:
        copy.wait()
    blocks = pair.shape[1]
    rows = routes.shape[1]
    length = rows // blocks
    pair_row = jnp.broadcast_to(pair[...], (blocks, blocks))
    ratio_row = jnp.broadcast_to(ratio[...], (blocks, blocks))
    length_row = jnp.broadcast_to(lengths[...], (blocks, blocks))
    eye = iota((blocks, blocks), 0) == iota((blocks, blocks), 1)
    pair_col = jnp.sum(jnp.where(eye, pair_row, 0), axis=1, keepdims=True)
    length_col = jnp.sum(jnp.where(eye, length_row, 0), axis=1, keepdims=True)
    chosen = jnp.sum(jnp.where(pair_row == (pair_col & -2), ratio_row, 0.0), axis=1, keepdims=True)
    refused = jnp.sum(jnp.where(pair_row == (pair_col | 1), ratio_row, 0.0), axis=1, keepdims=True)
    coef = BETA * jax.nn.sigmoid(-BETA * (chosen - refused))
    block_weight = jnp.where((pair_col & 1) == 0, -coef, coef)
    owner = iota((blocks, rows), 1) // length == iota((blocks, rows), 0)
    weight = jnp.sum(jnp.where(owner, block_weight, 0.0), axis=0, keepdims=True)
    valid = jnp.sum(jnp.where(owner, length_col, 0), axis=0, keepdims=True)
    live = iota((1, rows), 1) % length < valid
    weight = jnp.where(live, weight, 0.0)
    first, second = routes[0:1, :], routes[1:2, :]
    weight0, weight1 = combine[0:1, :] * weight, combine[1:2, :] * weight
    pad = -(-groups // 8) * 8
    label = iota((pad, rows), 0)
    counted = ((first == label) | (second == label)) & live
    counts = jnp.sum(jnp.where(counted, 1.0, 0.0), axis=1, keepdims=True)
    named = other(jnp.full((pad, rows), lax.axis_index("expert"), jnp.int32), label, groups)
    hit0, hit1 = first == named, second == named
    hit = hit0 | hit1
    before = jnp.where(iota((rows, rows), 0) < iota((rows, rows), 1), 1.0, 0.0).astype(BF16)
    rank = jnp.dot(jnp.where(hit, 1.0, 0.0).astype(BF16), before, preferred_element_type=F32)
    key = jnp.where(hit, rank, -1.0)
    by_group = jnp.where(hit0, weight0, jnp.where(hit1, weight1, 0.0))
    routed = jnp.where(label == 0, first, second).astype(F32)
    table[...] = jnp.concatenate(
        [key, by_group, routed, jnp.broadcast_to(counts, (pad, rows))], axis=0
    )
    copies[-1].wait()
    raw[...] = cot[:, : raw.shape[1]]
    place_scaled(most, key, by_group, cot[:, early:], scaled)


def place_scaled(most, key, by_group, source, outs):
    slot = iota((most, key.shape[1]), 0).astype(F32)
    for j, out in enumerate(outs):
        at = slot == key[j : j + 1, :]
        row_weight = jnp.sum(jnp.where(at, by_group[j : j + 1, :], 0.0), axis=1, keepdims=True)
        taken = jnp.dot(jnp.where(at, 1.0, 0.0).astype(BF16), source, preferred_element_type=F32)
        out[:most, :] = (row_weight * taken).astype(BF16)


def pack_early(most, line, table, *refs):
    source, outs = jnp.concatenate([x[...] for x in refs[:line]], axis=1), refs[line:]
    pad = table.shape[0] // 4
    place_scaled(most, table[:pad], table[pad : 2 * pad], source, outs)
    counts = split_counts(table[3 * pad :, :1], source.shape[1])
    for out in outs:
        out[most:, :] = counts


def split_counts(counts, columns):
    high = jnp.floor(counts * (1.0 / 128.0))
    both = jnp.concatenate([high, counts - 128.0 * high], axis=0)
    return jnp.broadcast_to(both, (both.shape[0], columns)).astype(BF16)


def read_counts(rows):
    rows = rows.astype(F32)
    half = rows.shape[0] // 2
    return 128.0 * rows[:half] + rows[half:]


def join_early(most, *refs):
    blocks, out = refs[:-1], refs[-1]
    counts = sum(read_counts(block[most:, :128]) for block in blocks)
    for i, block in enumerate(blocks):
        out[i * most : (i + 1) * most, :] = block[:most, :]
    out[len(blocks) * most :, :] = split_counts(counts[:, :1], out.shape[1])


def tally(rows, mine, theirs, out):
    out[...] = read_counts(mine[rows:, :128]) + read_counts(theirs[rows:, :128])


def pack_hidden(groups, most, hop, halves, table, hidden, *outs):
    rows, top, inner = hidden.shape
    width = inner // halves
    flat = rows * top
    part = other(lax.axis_index("dp"), hop, halves) if halves > 1 else 0
    columns = pl.ds(pl.multiple_of(part * width, 128), width)
    pad = table.shape[0] // 4
    key, routes = table[:pad], table[2 * pad : 3 * pad]
    spread = jnp.where(iota((rows, flat), 0) == iota((rows, flat), 1) // top, 1.0, 0.0).astype(BF16)
    high = jnp.floor(key * (1.0 / 16.0))
    named = [jnp.broadcast_to(routes[k : k + 1], (pad, rows)) for k in range(top)]
    stacked = jnp.concatenate([high, key - 16.0 * high] + named, axis=0).astype(BF16)
    wide = jnp.dot(stacked, spread, preferred_element_type=F32)
    key = 16.0 * wide[:pad] + wide[pad : 2 * pad]
    choice = iota((pad, flat), 1) % top
    route = wide[2 * pad : 3 * pad]
    for k in range(1, top):
        route = jnp.where(choice == k, wide[(2 + k) * pad : (3 + k) * pad], route)
    me = jnp.full((pad, flat), lax.axis_index("expert"), jnp.int32)
    label = other(me, iota((pad, flat), 0), groups).astype(F32)
    key = jnp.where(route == label, key, -1.0)
    slot = iota((most, flat), 0).astype(F32)
    source = hidden[:, :, columns].reshape(flat, width)
    for j in range(groups):
        at = jnp.where(slot == key[j : j + 1, :], 1.0, 0.0).astype(BF16)
        outs[j][...] = jnp.dot(at, source, preferred_element_type=F32).astype(BF16)


def turn(step, *refs):
    blocks, out, joined = refs[:-2], refs[-2], refs[-1]
    most = blocks[0].shape[0]
    for i, block in enumerate(blocks):
        joined[i * most : (i + 1) * most, :] = block[...]
    for i in range(0, joined.shape[0], step):
        out[:, i : i + step] = joined[i : i + step, :].T


def stack_into(out, parts):
    at = 0
    for part in parts:
        out[at : at + part.shape[0], :] = part[...]
        at += part.shape[0]


def join(*refs):
    stack_into(refs[-1], refs[:-1])


def pick(inner, outer, out):
    m = lax.axis_index("mp")
    at_end = (m == 0) | (m == lax.axis_size("mp") - 1)

    @pl.when(at_end)
    def _():
        out[...] = outer[...]

    @pl.when(jnp.logical_not(at_end))
    def _():
        out[...] = inner[...]


def shard_at(step):
    m = lax.axis_index("mp")
    low = m < 2
    return (m, m ^ 1, jnp.where(low, 2, 1), jnp.where(low, 3, 0))[step]


def half_product(tile, ht, mine, out):
    for i in range(0, ht.shape[0], tile):
        out[i : i + tile, :] = jnp.dot(
            ht[i : i + tile, :], mine[: ht.shape[1], :], preferred_element_type=F32
        )


def product(tile, line, steps, ht, *refs):
    count = len(steps)
    halves, theirs = refs[:count], refs[count : 2 * count]
    out, joined, total, sem = refs[-4:]
    rows = ht.shape[1]
    shard = out.shape[1] // line
    m = lax.axis_index("mp")
    marks, at = [], 0
    for step, x in zip(steps, theirs):
        width = x.shape[1]
        joined[:, at : at + width] = x[:rows, :]
        if step < 0:
            size = width // line
            marks += [(lax.rem(m + line - k, line) * shard, at + k * size, size) for k in range(line)]
        else:
            marks.append((shard_at(step) * shard + shard - width, at, width))
        at += width
    copies = []
    for i in range(0, ht.shape[0], tile):
        second = jnp.dot(ht[i : i + tile, :], joined[...], preferred_element_type=F32)
        at = 0
        for half in halves:
            columns = slice(at, at + half.shape[1])
            total[i : i + tile, columns] = half[i : i + tile, :] + second[:, columns]
            at += half.shape[1]
        for k, (column, at, size) in enumerate(marks):
            copy = pltpu.make_async_copy(
                total.at[pl.ds(i, tile), pl.ds(at, size)],
                out.at[pl.ds(i, tile), pl.ds(pl.multiple_of(column, 128), size)],
                sem.at[i // tile * len(marks) + k],
            )
            copy.start()
            copies.append(copy)
    for copy in copies:
        copy.wait()


def call(kernel, name, outs, specs, mib, flops, scratch=(), alias=None):
    many = isinstance(outs, list)
    moved = sum(math.prod(x.shape) * 4 for x in (outs if many else [outs]))
    return pl.pallas_call(
        kernel,
        out_shape=outs,
        in_specs=specs,
        out_specs=[VM] * len(outs) if many else (ANY if "_product" in name else VM),
        scratch_shapes=list(scratch),
        input_output_aliases=alias or {},
        compiler_params=pltpu.CompilerParams(vmem_limit_bytes=mib << 20),
        cost_estimate=pl.CostEstimate(flops=flops, bytes_accessed=moved, transcendentals=0),
    )


def work(hidden, cotangent, routes, combine, block_pair, lengths, log_ratio):
    dp, groups, line = (lax.axis_size(name) for name in ("dp", "expert", "mp"))
    tokens, top = routes.shape
    most = 3 * tokens // 4
    full = cotangent.shape[1]
    inner = hidden.shape[2]
    fast = dp == 2 and line == 4 and full % 512 == 0 and inner % 256 == 0
    halves = 2 if fast else 1
    part = inner // halves
    early = full // 4 if fast else 0
    width = full - early
    rows = groups * most
    pad = 8 * (-(-groups // 8))
    operands = (routes.T, combine.T, block_pair, lengths, log_ratio, cotangent)

    packed = call(
        functools.partial(pack_scaled, groups, most, early),
        "pack_scaled",
        [
            jax.ShapeDtypeStruct((4 * pad, tokens), F32),
            jax.ShapeDtypeStruct((tokens, max(early, 128)), BF16),
        ]
        + [jax.ShapeDtypeStruct((most, width), BF16)] * groups,
        [HBM] * 6,
        60,
        2 * groups * most * tokens * width,
        [pltpu.VMEM(x.shape, x.dtype) for x in operands] + [pltpu.SemaphoreType.DMA((6,))],
    )(*operands)
    table, raw = packed[:2]
    scaled = packed[2:]

    packed_h = [
        call(
            functools.partial(pack_hidden, groups, most, h, halves),
            f"pack_hidden{h}",
            [jax.ShapeDtypeStruct((most, part), BF16)] * groups,
            [VM, VM],
            24,
            2 * rows * tokens * top * part,
        )(table, hidden)
        for h in range(halves)
    ]

    arrived = [scaled[0]] + [
        lax.ppermute(scaled[j], "expert", pairs_of(groups, j)) for j in range(1, groups)
    ]
    blocks = []
    for h in range(halves):
        for j in range(groups):
            block = packed_h[h][j]
            if h:
                block = lax.ppermute(
                    block,
                    ("dp", "expert"),
                    [(a * groups + b, (a ^ h) * groups + c) for a in range(dp) for b, c in pairs_of(groups, j)],
                )
            elif j:
                block = lax.ppermute(block, "expert", pairs_of(groups, j))
            blocks.append(block)

    start = call(
        join, "join", jax.ShapeDtypeStruct((rows, width), BF16), [VM] * groups, 8, 0
    )(*arrived)
    if not fast:
        expert_load = lax.psum(table[3 * pad : 3 * pad + groups, 0], ("dp", "expert"))
        gathered = lax.all_gather(start, "mp", axis=1, tiled=True)
        partial = lax.dot_general(
            jnp.concatenate(blocks, axis=0),
            gathered,
            (((0,), (0,)), ((), ())),
            preferred_element_type=F32,
        )
        owned = lax.psum_scatter(partial, "dp", scatter_dimension=0, tiled=True)
        return owned[None], expert_load

    pairs, middle, outward = [(0, 1), (1, 0), (2, 3), (3, 2)], [(1, 2), (2, 1)], [(1, 0), (2, 3)]
    p1, q1 = lax.ppermute(start, "mp", pairs), lax.ppermute(start, "mp", middle)
    q2, p2 = lax.ppermute(p1, "mp", middle), lax.ppermute(q1, "mp", outward)
    p3 = lax.ppermute(q2, "mp", outward)

    def picked(name, inner_rows, outer_rows):
        return call(pick, name, jax.ShapeDtypeStruct((rows, width), BF16), [VM] * 2, 8, 0)(
            inner_rows, outer_rows
        )

    shards = [start, p1, picked("pick2", q1, p2), picked("pick3", q2, p3)]

    step = 128 if rows % 128 == 0 else most
    turned = [
        call(
            functools.partial(turn, step),
            f"turn{h}",
            jax.ShapeDtypeStruct((part, rows), BF16),
            [VM] * groups,
            12,
            rows * part * 512,
            [pltpu.VMEM((rows, part), BF16)],
        )(*blocks[h * groups : (h + 1) * groups])
        for h in range(halves)
    ]
    tile = part // 4 if part % 32 == 0 else part
    out_shape = jax.ShapeDtypeStruct((part, full * line), F32)

    def swap(mine):
        return lax.ppermute(mine, "dp", [(0, 1), (1, 0)])

    def half(name, mine):
        return call(
            functools.partial(half_product, tile),
            name,
            jax.ShapeDtypeStruct((part, mine.shape[1]), F32),
            [VM, VM],
            12,
            2 * part * rows * mine.shape[1],
        )(turned[0], mine)

    def finish(name, halves, theirs, steps, out):
        columns = sum(x.shape[1] for x in theirs)
        writes = len(steps) + (line - 1 if -1 in steps else 0)
        extra = [] if out is None else [out]
        return call(
            functools.partial(product, tile, line, steps),
            name,
            out_shape,
            [VM] * (1 + 2 * len(theirs)) + [ANY] * len(extra),
            20,
            2 * part * rows * columns,
            [
                pltpu.VMEM((rows, columns), BF16),
                pltpu.VMEM((part, columns), F32),
                pltpu.SemaphoreType.DMA((part // tile * writes,)),
            ],
            {} if out is None else {1 + 2 * len(theirs): 0},
        )(turned[1], *halves, *theirs, *extra)

    own = [half(f"half{i}", x) for i, x in enumerate(shards)]
    theirs = [swap(x) for x in shards]
    out = finish("pair_product", own[:2], theirs[:2], (0, 1), None)
    out = finish("next_product", own[2:3], theirs[2:3], (2,), out)
    spread = [raw] + [
        lax.ppermute(raw, "mp", [(a, (a + k) % line) for a in range(line)])
        for k in range(1, line)
    ]
    sent = call(
        functools.partial(pack_early, most, line),
        "pack_early",
        [jax.ShapeDtypeStruct((most + 2 * pad, early * line), BF16)] * groups,
        [VM] * (1 + line),
        12,
        2 * rows * tokens * early * line,
    )(table, *spread)
    kept = [sent[0]] + [
        lax.ppermute(sent[j], "expert", pairs_of(groups, j)) for j in range(1, groups)
    ]
    mine = call(
        functools.partial(join_early, most),
        "join_early",
        jax.ShapeDtypeStruct((rows + 2 * pad, early * line), BF16),
        [VM] * groups,
        8,
        0,
    )(*kept)
    other_core = swap(mine)
    out = finish(
        "last_product",
        [half("half_early", mine), own[3]],
        [other_core, theirs[3]],
        (-1, 3),
        out,
    )
    expert_load = call(
        functools.partial(tally, rows),
        "tally",
        jax.ShapeDtypeStruct((pad, 128), F32),
        [VM] * 2,
        8,
        0,
    )(mine, other_core)[:groups, 0]
    return out[None], expert_load


def solution(mesh):
    in_specs = (
        P(("dp", "expert"), None, "mp"),
        P(("dp", "expert"), "mp"),
        P(("dp", "expert"), None),
        P(("dp", "expert"), None),
        P(("dp", "expert"), None),
        P(("dp", "expert"), None),
        P(("dp", "expert"), None),
    )
    out_specs = (P("expert", ("mp", "dp"), None), P())
    step = jax.shard_map(work, mesh=mesh, in_specs=in_specs, out_specs=out_specs, check_vma=False)
    if tuple(mesh.shape[name] for name in ("dp", "expert", "mp")) != (2, 4, 4):
        return step
    return step
```

```python
import functools
import math
import jax
import jax.numpy as jnp
from jax import lax
from jax.experimental import pallas as pl
from jax.experimental.pallas import tpu as pltpu
from jax.sharding import PartitionSpec as P


BETA = 0.1
F32 = jnp.float32
BF16 = jnp.bfloat16
VM = pl.BlockSpec(memory_space=pltpu.VMEM)
ANY = pl.BlockSpec(memory_space=pl.ANY)
HBM = pl.BlockSpec(memory_space=pltpu.HBM)


def iota(shape, dim):
    return lax.broadcasted_iota(jnp.int32, shape, dim)


def other(place, hop, size):
    return place ^ hop if size & (size - 1) == 0 else lax.rem(place + hop, size)


def pairs_of(size, hop):
    return [(i, i ^ hop if size & (size - 1) == 0 else (i + hop) % size) for i in range(size)]


def pack_scaled(groups, most, early, *refs):
    table, raw = refs[6:8]
    scaled = refs[8 : 8 + groups]
    routes, combine, pair, lengths, ratio, cot, sem = refs[8 + groups :]
    copies = [
        pltpu.make_async_copy(source, held, sem.at[i])
        for i, (source, held) in enumerate(zip(refs[:6], (routes, combine, pair, lengths, ratio, cot)))
    ]
    for copy in copies:
        copy.start()
    for copy in copies[:-1]:
        copy.wait()
    blocks = pair.shape[1]
    rows = routes.shape[1]
    length = rows // blocks
    pair_row = jnp.broadcast_to(pair[...], (blocks, blocks))
    ratio_row = jnp.broadcast_to(ratio[...], (blocks, blocks))
    length_row = jnp.broadcast_to(lengths[...], (blocks, blocks))
    eye = iota((blocks, blocks), 0) == iota((blocks, blocks), 1)
    pair_col = jnp.sum(jnp.where(eye, pair_row, 0), axis=1, keepdims=True)
    length_col = jnp.sum(jnp.where(eye, length_row, 0), axis=1, keepdims=True)
    chosen = jnp.sum(jnp.where(pair_row == (pair_col & -2), ratio_row, 0.0), axis=1, keepdims=True)
    refused = jnp.sum(jnp.where(pair_row == (pair_col | 1), ratio_row, 0.0), axis=1, keepdims=True)
    coef = BETA * jax.nn.sigmoid(-BETA * (chosen - refused))
    block_weight = jnp.where((pair_col & 1) == 0, -coef, coef)
    owner = iota((blocks, rows), 1) // length == iota((blocks, rows), 0)
    weight = jnp.sum(jnp.where(owner, block_weight, 0.0), axis=0, keepdims=True)
    valid = jnp.sum(jnp.where(owner, length_col, 0), axis=0, keepdims=True)
    live = iota((1, rows), 1) % length < valid
    weight = jnp.where(live, weight, 0.0)
    first, second = routes[0:1, :], routes[1:2, :]
    weight0, weight1 = combine[0:1, :] * weight, combine[1:2, :] * weight
    pad = -(-groups // 8) * 8
    label = iota((pad, rows), 0)
    counted = ((first == label) | (second == label)) & live
    counts = jnp.sum(jnp.where(counted, 1.0, 0.0), axis=1, keepdims=True)
    named = other(jnp.full((pad, rows), lax.axis_index("expert"), jnp.int32), label, groups)
    hit0, hit1 = first == named, second == named
    hit = hit0 | hit1
    before = jnp.where(iota((rows, rows), 0) < iota((rows, rows), 1), 1.0, 0.0).astype(BF16)
    rank = jnp.dot(jnp.where(hit, 1.0, 0.0).astype(BF16), before, preferred_element_type=F32)
    key = jnp.where(hit, rank, -1.0)
    by_group = jnp.where(hit0, weight0, jnp.where(hit1, weight1, 0.0))
    routed = jnp.where(label == 0, first, second).astype(F32)
    table[...] = jnp.concatenate(
        [key, by_group, routed, jnp.broadcast_to(counts, (pad, rows))], axis=0
    )
    copies[-1].wait()
    raw[...] = cot[:, : raw.shape[1]]
    place_scaled(most, key, by_group, cot[:, early:], scaled)


def place_scaled(most, key, by_group, source, outs):
    slot = iota((most, key.shape[1]), 0).astype(F32)
    for j, out in enumerate(outs):
        at = slot == key[j : j + 1, :]
        row_weight = jnp.sum(jnp.where(at, by_group[j : j + 1, :], 0.0), axis=1, keepdims=True)
        taken = jnp.dot(jnp.where(at, 1.0, 0.0).astype(BF16), source, preferred_element_type=F32)
        out[:most, :] = (row_weight * taken).astype(BF16)


def pack_early(most, line, table, *refs):
    source, outs = jnp.concatenate([x[...] for x in refs[:line]], axis=1), refs[line:]
    pad = table.shape[0] // 4
    place_scaled(most, table[:pad], table[pad : 2 * pad], source, outs)
    counts = split_counts(table[3 * pad :, :1], source.shape[1])
    for out in outs:
        out[most:, :] = counts


def split_counts(counts, columns):
    high = jnp.floor(counts * (1.0 / 128.0))
    both = jnp.concatenate([high, counts - 128.0 * high], axis=0)
    return jnp.broadcast_to(both, (both.shape[0], columns)).astype(BF16)


def read_counts(rows):
    rows = rows.astype(F32)
    half = rows.shape[0] // 2
    return 128.0 * rows[:half] + rows[half:]


def join_early(most, *refs):
    blocks, out = refs[:-1], refs[-1]
    counts = sum(read_counts(block[most:, :128]) for block in blocks)
    for i, block in enumerate(blocks):
        out[i * most : (i + 1) * most, :] = block[:most, :]
    out[len(blocks) * most :, :] = split_counts(counts[:, :1], out.shape[1])


def tally(rows, mine, theirs, out):
    out[...] = read_counts(mine[rows:, :128]) + read_counts(theirs[rows:, :128])


def pack_hidden(groups, most, hop, halves, table, hidden, *rest):
    outs, held, sem = rest[:groups], rest[groups], rest[groups + 1]
    rows, top, width = held.shape
    flat = rows * top
    part = other(lax.axis_index("dp"), hop, halves) if halves > 1 else 0
    columns = pl.ds(pl.multiple_of(part * width, 128), width)
    copy = pltpu.make_async_copy(hidden.at[:, :, columns], held, sem)
    copy.start()
    pad = table.shape[0] // 4
    key, routes = table[:pad], table[2 * pad : 3 * pad]
    spread = jnp.where(iota((rows, flat), 0) == iota((rows, flat), 1) // top, 1.0, 0.0).astype(BF16)
    high = jnp.floor(key * (1.0 / 16.0))
    named = [jnp.broadcast_to(routes[k : k + 1], (pad, rows)) for k in range(top)]
    stacked = jnp.concatenate([high, key - 16.0 * high] + named, axis=0).astype(BF16)
    wide = jnp.dot(stacked, spread, preferred_element_type=F32)
    key = 16.0 * wide[:pad] + wide[pad : 2 * pad]
    choice = iota((pad, flat), 1) % top
    route = wide[2 * pad : 3 * pad]
    for k in range(1, top):
        route = jnp.where(choice == k, wide[(2 + k) * pad : (3 + k) * pad], route)
    me = jnp.full((pad, flat), lax.axis_index("expert"), jnp.int32)
    label = other(me, iota((pad, flat), 0), groups).astype(F32)
    key = jnp.where(route == label, key, -1.0)
    slot = iota((most, flat), 0).astype(F32)
    copy.wait()
    source = held[...].reshape(flat, width)
    for j in range(groups):
        at = jnp.where(slot == key[j : j + 1, :], 1.0, 0.0).astype(BF16)
        outs[j][...] = jnp.dot(at, source, preferred_element_type=F32).astype(BF16)


def turn(step, *refs):
    blocks, out, joined = refs[:-2], refs[-2], refs[-1]
    most = blocks[0].shape[0]
    for i, block in enumerate(blocks):
        joined[i * most : (i + 1) * most, :] = block[...]
    for i in range(0, joined.shape[0], step):
        out[:, i : i + step] = joined[i : i + step, :].T


def stack_into(out, parts):
    at = 0
    for part in parts:
        out[at : at + part.shape[0], :] = part[...]
        at += part.shape[0]


def join(*refs):
    stack_into(refs[-1], refs[:-1])


def pick(inner, outer, out):
    m = lax.axis_index("mp")
    at_end = (m == 0) | (m == lax.axis_size("mp") - 1)

    @pl.when(at_end)
    def _():
        out[...] = outer[...]

    @pl.when(jnp.logical_not(at_end))
    def _():
        out[...] = inner[...]


def shard_at(step):
    m = lax.axis_index("mp")
    low = m < 2
    return (m, m ^ 1, jnp.where(low, 2, 1), jnp.where(low, 3, 0))[step]


def split(source, *outs):
    at = 0
    for out in outs:
        out[...] = source[at : at + out.shape[0], :]
        at += out.shape[0]


def partial_product(tile, offsets, *refs):
    out, pairs = refs[-1], refs[: 2 * len(offsets)]
    earlier = refs[2 * len(offsets) : -1]
    for i in range(0, out.shape[0], tile):
        total = sum(x[i : i + tile, :] for x in earlier)
        for k, offset in enumerate(offsets):
            ht, x = pairs[2 * k : 2 * k + 2]
            count = min(ht.shape[1] - offset, x.shape[0])
            total += jnp.dot(
                ht[i : i + tile, offset : offset + count], x[:count, :], preferred_element_type=F32
            )
        out[i : i + tile, :] = total


def product(tile, line, steps, ht, *refs):
    count = len(steps)
    halves, theirs = refs[:count], refs[count : 2 * count]
    out, joined, total, sem = refs[-4:]
    rows = ht.shape[1]
    shard = out.shape[1] // line
    m = lax.axis_index("mp")
    marks, at, spans = [], 0, []
    for step, x in zip(steps, theirs):
        width = x.shape[1]
        spans.append((rows - min(rows, x.shape[0]), at, at + width))
        count_of = min(rows, x.shape[0])
        joined[rows - count_of :, at : at + width] = x[:count_of, :]
        if step < 0:
            size = width // line
            marks += [(lax.rem(m + line - k, line) * shard, at + k * size, size) for k in range(line)]
        else:
            marks.append((shard_at(step) * shard + shard - width, at, width))
        at += width
    copies = []
    for i in range(0, ht.shape[0], tile):
        if all(skip == 0 for skip, _, _ in spans):
            both = jnp.dot(ht[i : i + tile, :], joined[...], preferred_element_type=F32)
            second = [both[:, low:high] for _, low, high in spans]
        else:
            second = [
                jnp.dot(ht[i : i + tile, skip:], joined[skip:, low:high], preferred_element_type=F32)
                for skip, low, high in spans
            ]
        for half, rest, (_, low, high) in zip(halves, second, spans):
            total[i : i + tile, low:high] = half[i : i + tile, :] + rest
        for k, (column, at, size) in enumerate(marks):
            copy = pltpu.make_async_copy(
                total.at[pl.ds(i, tile), pl.ds(at, size)],
                out.at[pl.ds(i, tile), pl.ds(pl.multiple_of(column, 128), size)],
                sem.at[i // tile * len(marks) + k],
            )
            copy.start()
            copies.append(copy)
    for copy in copies:
        copy.wait()


def call(kernel, name, outs, specs, mib, flops, scratch=(), alias=None):
    many = isinstance(outs, list)
    moved = sum(math.prod(x.shape) * 4 for x in (outs if many else [outs]))
    return pl.pallas_call(
        kernel,
        out_shape=outs,
        in_specs=specs,
        out_specs=[VM] * len(outs) if many else (ANY if "_product" in name else VM),
        scratch_shapes=list(scratch),
        input_output_aliases=alias or {},
        compiler_params=pltpu.CompilerParams(vmem_limit_bytes=mib << 20),
        cost_estimate=pl.CostEstimate(flops=flops, bytes_accessed=moved, transcendentals=0),
    )


def work(hidden, cotangent, routes, combine, block_pair, lengths, log_ratio):
    dp, groups, line = (lax.axis_size(name) for name in ("dp", "expert", "mp"))
    tokens, top = routes.shape
    most = 3 * tokens // 4
    full = cotangent.shape[1]
    inner = hidden.shape[2]
    fast = dp == 2 and line == 4 and full % 512 == 0 and inner % 256 == 0
    halves = 2 if fast else 1
    part = inner // halves
    early = full // 4 if fast else 0
    width = full - early
    rows = groups * most
    pad = 8 * (-(-groups // 8))
    operands = (routes.T, combine.T, block_pair, lengths, log_ratio, cotangent)
    operands = tuple(pltpu.with_memory_space_constraint(x, pltpu.HBM) for x in operands)
    hidden = pltpu.with_memory_space_constraint(hidden, pltpu.HBM)

    packed = call(
        functools.partial(pack_scaled, groups, most, early),
        "pack_scaled",
        [
            jax.ShapeDtypeStruct((4 * pad, tokens), F32),
            jax.ShapeDtypeStruct((tokens, max(early, 128)), BF16),
        ]
        + [jax.ShapeDtypeStruct((most, width), BF16)] * groups,
        [HBM] * 6,
        12,
        2 * groups * most * tokens * width,
        [pltpu.VMEM(x.shape, x.dtype) for x in operands] + [pltpu.SemaphoreType.DMA((6,))],
    )(*operands)
    table, raw = packed[:2]
    scaled = packed[2:]

    packed_h = [
        call(
            functools.partial(pack_hidden, groups, most, h, halves),
            f"pack_hidden{h}",
            [jax.ShapeDtypeStruct((most, part), BF16)] * groups,
            [VM, HBM],
            24,
            2 * rows * tokens * top * part,
            [pltpu.VMEM((tokens, top, part), BF16), pltpu.SemaphoreType.DMA],
        )(table, hidden)
        for h in range(halves)
    ]

    arrived = [scaled[0]] + [
        lax.ppermute(scaled[j], "expert", pairs_of(groups, j)) for j in range(1, groups)
    ]
    blocks = []
    for h in range(halves):
        for j in range(groups):
            block = packed_h[h][j]
            if h:
                block = lax.ppermute(
                    block,
                    ("dp", "expert"),
                    [(a * groups + b, (a ^ h) * groups + c) for a in range(dp) for b, c in pairs_of(groups, j)],
                )
            elif j:
                block = lax.ppermute(block, "expert", pairs_of(groups, j))
            blocks.append(block)

    start = call(
        join, "join", jax.ShapeDtypeStruct((rows, width), BF16), [VM] * groups, 8, 0
    )(*arrived)
    if not fast:
        expert_load = lax.psum(table[3 * pad : 3 * pad + groups, 0], ("dp", "expert"))
        gathered = lax.all_gather(start, "mp", axis=1, tiled=True)
        partial = lax.dot_general(
            jnp.concatenate(blocks, axis=0),
            gathered,
            (((0,), (0,)), ((), ())),
            preferred_element_type=F32,
        )
        owned = lax.psum_scatter(partial, "dp", scatter_dimension=0, tiled=True)
        return owned[None], expert_load

    pairs, middle, outward = [(0, 1), (1, 0), (2, 3), (3, 2)], [(1, 2), (2, 1)], [(1, 0), (2, 3)]
    p1, q1 = lax.ppermute(start, "mp", pairs), lax.ppermute(start, "mp", middle)
    cut = rows // 2
    p1a, p1b = call(
        split, "split", [jax.ShapeDtypeStruct((cut, width), BF16)] * 2, [VM], 8, 0
    )(p1)
    q2a, q2b = lax.ppermute(p1a, "mp", middle), lax.ppermute(p1b, "mp", middle)
    p2 = lax.ppermute(q1, "mp", outward)
    p3a, p3b = lax.ppermute(q2a, "mp", outward), lax.ppermute(q2b, "mp", outward)

    def picked(name, inner_rows, outer_rows):
        return call(pick, name, jax.ShapeDtypeStruct(inner_rows.shape, BF16), [VM] * 2, 8, 0)(
            inner_rows, outer_rows
        )

    shards = [start, p1, picked("pick2", q1, p2)]
    last_a, last_b = picked("pick_a", q2a, p3a), picked("pick_b", q2b, p3b)

    step = 128 if rows % 128 == 0 else most
    turned = [
        call(
            functools.partial(turn, step),
            f"turn{h}",
            jax.ShapeDtypeStruct((part, rows), BF16),
            [VM] * groups,
            12,
            rows * part * 512,
            [pltpu.VMEM((rows, part), BF16)],
        )(*blocks[h * groups : (h + 1) * groups])
        for h in range(halves)
    ]
    tile = part // 4 if part % 32 == 0 else part
    out_shape = jax.ShapeDtypeStruct((part, full * line), F32)

    def swap(mine):
        return lax.ppermute(mine, "dp", [(0, 1), (1, 0)])

    def accumulate(name, pairs, offsets, *earlier):
        columns = pairs[0][1].shape[1]
        return call(
            functools.partial(partial_product, tile, offsets),
            name,
            jax.ShapeDtypeStruct((part, columns), F32),
            [VM] * (2 * len(pairs) + len(earlier)),
            16,
            2 * part * cut * columns * len(pairs),
        )(*[x for pair in pairs for x in pair], *earlier)

    def half(name, mine):
        return accumulate(name, [(turned[0], mine)], (0,))

    def finish(name, halves, theirs, steps, out):
        columns = sum(x.shape[1] for x in theirs)
        writes = len(steps) + (line - 1 if -1 in steps else 0)
        extra = [] if out is None else [out]
        return call(
            functools.partial(product, tile, line, steps),
            name,
            out_shape,
            [VM] * (1 + 2 * len(theirs)) + [ANY] * len(extra),
            20,
            2 * part * rows * columns,
            [
                pltpu.VMEM((rows, columns), BF16),
                pltpu.VMEM((part, columns), F32),
                pltpu.SemaphoreType.DMA((part // tile * writes,)),
            ],
            {} if out is None else {1 + 2 * len(theirs): 0},
        )(turned[1], *halves, *theirs, *extra)

    own = [half(f"half{i}", x) for i, x in enumerate(shards)]
    theirs = [swap(x) for x in shards]
    out = finish("pair_product", own[:2], theirs[:2], (0, 1), None)
    out = finish("next_product", own[2:3], theirs[2:3], (2,), out)
    spread = [raw] + [
        lax.ppermute(raw, "mp", [(a, (a + k) % line) for a in range(line)])
        for k in range(1, line)
    ]
    sent = call(
        functools.partial(pack_early, most, line),
        "pack_early",
        [jax.ShapeDtypeStruct((most + 2 * pad, early * line), BF16)] * groups,
        [VM] * (1 + line),
        12,
        2 * rows * tokens * early * line,
    )(table, *spread)
    kept = [sent[0]] + [
        lax.ppermute(sent[j], "expert", pairs_of(groups, j)) for j in range(1, groups)
    ]
    mine = call(
        functools.partial(join_early, most),
        "join_early",
        jax.ShapeDtypeStruct((rows + 2 * pad, early * line), BF16),
        [VM] * groups,
        8,
        0,
    )(*kept)
    other_core = swap(mine)
    half_early = half("half_early", mine)
    last = accumulate("half3a", [(turned[0], last_a), (turned[1], swap(last_a))], (0, 0))
    last = accumulate("half3b", [(turned[0], last_b)], (cut,), last)
    out = finish("last_product", [half_early, last], [other_core, swap(last_b)], (-1, 3), out)
    expert_load = call(
        functools.partial(tally, rows),
        "tally",
        jax.ShapeDtypeStruct((pad, 128), F32),
        [VM] * 2,
        8,
        0,
    )(mine, other_core)[:groups, 0]
    return out[None], expert_load


def solution(mesh):
    in_specs = (
        P(("dp", "expert"), None, "mp"),
        P(("dp", "expert"), "mp"),
        P(("dp", "expert"), None),
        P(("dp", "expert"), None),
        P(("dp", "expert"), None),
        P(("dp", "expert"), None),
        P(("dp", "expert"), None),
    )
    out_specs = (P("expert", ("mp", "dp"), None), P())
    step = jax.shard_map(work, mesh=mesh, in_specs=in_specs, out_specs=out_specs, check_vma=False)
    if tuple(mesh.shape[name] for name in ("dp", "expert", "mp")) != (2, 4, 4):
        return step
    return step
```
